32 devices in a mesh: grp: 2 (over y), row: 4 (over z), col: 4 (over x, core).
Axes of the slice: x: 2, y: 2, z: 4, core: 2. Of those that a mesh axis runs over, the one named last changes fastest.
Arguments:
- z_spectra: float32 [32, 2, 2, 4096], P(('grp', 'row', 'col')), parts along dimension 0, may hold values from -6 to 6
- n_spectra: float32 [32, 2, 2, 4096], P(('grp', 'col', 'row')), parts along dimension 0, may hold values from -6 to 6
- z_flags: int32 [32, 2], P(('grp', 'row', 'col')), parts along dimension 0, may hold values 0 or 1
- n_flags: int32 [32, 2], P(('grp', 'col', 'row')), parts along dimension 0, may hold values 0 or 1
- pair_mask: int32 [32, 16], P(('grp', 'row'), 'col'), parts along dimension 0, may hold values 0 or 1
Outputs:
- stacks: float32 [32, 16, 512], P(('grp', 'row'), 'col'), parts along dimension 0
The draws below stay inside these ranges and needn't reach their ends.
There are 2 independent parts, one for each index of `grp`. The reference program is written for one: setup_inputs(seed, part) draws one part's arguments, and reference() takes and returns one part's arrays. A program takes and returns all parts, laid end to end along the dimension named above; each array names one. Nothing has to cross between parts.
All inputs are finite; a program needn't handle non-finite values. No bound on the sum of `z_flags` or of `n_flags` or of `pair_mask` on one device may be relied on, other than what follows from the above.
Results may differ from the reference program's by a relative error of at most 0.0037.
Values sent between devices are 32-bit elements; how exact they have to be, the bound alone decides.
No kernel may reach another device: no remote copies, remote signals or barrier semaphores. Data moves between devices by JAX's collectives and lax.ppermute only.
A program may use at most 64 MiB of HBM per device.

```python
import math
import jax
import jax.numpy as jnp
from jax import lax

F = 4096
LAGS = 512
WIN = 2
S = 16


def place_ends(drawn, own_key, smallest, high):
    longest = drawn.shape.index(max(drawn.shape))
    spots = []
    for shift in (0, 1):
        where = [jax.random.randint(jax.random.fold_in(own_key, axis), (), 0, length) for axis, length in enumerate(drawn.shape)]
        where[longest] = (where[longest] + shift) % drawn.shape[longest]
        spots.append(tuple(where))
    return drawn.at[spots[0]].set(smallest).at[spots[1]].set(high)


def block_levels(stream_key, shape, pieces, least, high):
    def one(dim, blocks):
        steps = jax.random.uniform(jax.random.fold_in(jax.random.fold_in(stream_key, 6), dim), (blocks,), jnp.float32, least / len(pieces), high / len(pieces))
        return jnp.repeat(jnp.exp(steps), shape[dim] // blocks).reshape((-1,) + (1,) * (len(shape) - dim - 1))

    gain = one(*pieces[0])
    for cut in pieces[1:]:
        gain = gain * one(*cut)
    return gain


def scatter_about(stream_key, dims, scale, most, pieces=(), kind=jnp.bfloat16):
    loudness = block_levels(stream_key, dims, pieces, -0.22, 0.18) if pieces else 1.0
    array = jax.random.normal(stream_key, dims, jnp.float32) * scale * loudness
    return jnp.minimum(jnp.maximum(array, -most), most).astype(kind)


def setup_inputs(seed: int = 0, part: int = 0) -> dict:
    streams_of = jax.random.split(jax.random.key(seed), 6)
    part_splits = jax.random.split(jax.random.fold_in(streams_of[5], part), 6)
    z_spectra = scatter_about(part_splits[0], (S, WIN, 2, F), 1.0, 6.0, ((0, 16),), jnp.float32)
    n_spectra = scatter_about(part_splits[1], (S, WIN, 2, F), 1.0, 6.0, ((0, 16),), jnp.float32)
    z_flags = place_ends((jax.random.randint(part_splits[2], (S, WIN), 0, 5) < 4).astype(jnp.int32), jax.random.fold_in(part_splits[2], 1), 0, 1)
    n_flags = place_ends((jax.random.randint(part_splits[3], (S, WIN), 0, 5) < 4).astype(jnp.int32), jax.random.fold_in(part_splits[3], 1), 0, 1)
    pair_mask = place_ends((jax.random.randint(part_splits[4], (S, S), 0, 4) < 3).astype(jnp.int32), jax.random.fold_in(part_splits[4], 1), 0, 1)
    return {"z_spectra": z_spectra, "n_spectra": n_spectra, "z_flags": z_flags, "n_flags": n_flags, "pair_mask": pair_mask}


def lag_table(first_bin, bin_count, total_bins, lag_count):
    freq_bins = first_bin + jnp.arange(bin_count, dtype=jnp.int32)
    lag_steps = jnp.arange(lag_count, dtype=jnp.int32) - lag_count // 2
    phase_index = freq_bins[:, None] * lag_steps[None, :] % (2 * total_bins)
    angles = phase_index.astype(jnp.float32) * (math.pi / total_bins)
    weight = jnp.where(freq_bins == 0, 1.0, 2.0).astype(jnp.float32)[:, None]
    return jnp.concatenate([weight * jnp.cos(angles), -weight * jnp.sin(angles)], 0).astype(jnp.bfloat16)

def correlate(row_spec, col_spec, lag_tab):
    z_real = row_spec[:, None, :, 0, :]
    z_imag = row_spec[:, None, :, 1, :]
    n_real = col_spec[None, :, :, 0, :]
    n_imag = col_spec[None, :, :, 1, :]
    real_part = z_real * n_real + z_imag * n_imag
    imag_part = z_imag * n_real - z_real * n_imag
    row_count, col_count, windows, bins = real_part.shape
    cross_spec = jnp.stack([real_part, imag_part], 3).astype(jnp.bfloat16)
    merged = cross_spec.reshape(row_count * col_count * windows, 2 * bins)
    product = jnp.dot(merged, lag_tab, preferred_element_type=jnp.float32)
    return product.reshape(row_count, col_count, windows, lag_tab.shape[1])

def stack_windows(corr, pair_marks):
    spread = jnp.sqrt(lax.optimization_barrier(jnp.mean(corr * corr, -1, keepdims=True)) + 1e-05)
    unit_corr = corr / spread
    window_count = jnp.maximum(lax.optimization_barrier(jnp.sum(pair_marks, -1)), 1.0)
    summed = lax.optimization_barrier(jnp.sum(pair_marks[..., None] * unit_corr, -2))
    return summed / window_count[..., None]

def reference(z_spectra, n_spectra, z_flags, n_flags, pair_mask):
    lag_tab = lag_table(0, F, F, LAGS)
    z_marks = z_flags.astype(jnp.float32)
    n_marks = n_flags.astype(jnp.float32)

    def one_station(inputs):
        z_row, z_mark = inputs
        corr = correlate(z_row[None], n_spectra, lag_tab)[0]
        return stack_windows(corr, z_mark[None, :] * n_marks)
    stacked = lax.map(one_station, (z_spectra, z_marks))
    return stacked * pair_mask.astype(jnp.float32)[..., None]
```

```python
import functools
import math

import jax
import jax.numpy as jnp
import numpy as np
from jax import lax
from jax.experimental import pallas as pl
from jax.experimental.pallas import tpu as pltpu
from jax.sharding import PartitionSpec as P

LAGS = 512
LANES = 128
DEPTH = 2 * LANES


def load_parts(ref, window, groups):
    base = window * 4 * groups
    return [ref[pl.ds(base + k, groups, stride=4), :] for k in (0, 2, 1, 3)]


def spread(ref, i, j, count):
    return jnp.broadcast_to(ref[i : i + 1, j : j + 1].astype(jnp.float32), (count, LANES))


def prepare_kernel(groups, lags, coarse_ref, fine_ref, inner_ref):
    steps = fine_ref.shape[0]
    fine_cos, fine_sin = fine_ref[:, :lags], fine_ref[:, lags:]
    for k in range(coarse_ref.shape[0]):
        coarse_cos, coarse_sin = coarse_ref[k : k + 1, :lags], coarse_ref[k : k + 1, lags:]
        cos = (coarse_cos * fine_cos - coarse_sin * fine_sin).astype(jnp.bfloat16)
        sin = (coarse_sin * fine_cos + coarse_cos * fine_sin).astype(jnp.bfloat16)
        top, low = pl.ds(k * steps, steps), pl.ds(DEPTH + k * steps, steps)
        inner_ref[top, :lags] = cos
        inner_ref[top, lags:] = sin
        inner_ref[low, :lags] = (0.0 - sin.astype(jnp.float32)).astype(jnp.bfloat16)
        inner_ref[low, lags:] = cos


def correlate_kernel(axes, z_count, n_count, windows, groups, lags, *refs):
    z_refs, refs = refs[:z_count], refs[z_count:]
    n_refs, refs = refs[:n_count], refs[n_count:]
    zf_refs, refs = refs[:z_count], refs[z_count:]
    nf_refs, refs = refs[:n_count], refs[n_count:]
    inner_ref, outer_ref, mask_ref, out_ref, lhs_ref, rows_ref = refs
    row = lax.broadcasted_iota(jnp.int32, (groups, LANES), 0)
    lane = lax.broadcasted_iota(jnp.int32, (groups, LANES), 1)
    first = jnp.where((row == 0) & (lane == 0), 0.5, 1.0)
    pairs = z_count * n_count
    for w in range(windows):
        for a in range(z_count):
            zr0, zr1, zi0, zi1 = load_parts(z_refs[a], w, groups)
            zr0, zi0 = zr0 * first, zi0 * first
            for b in range(n_count):
                nr0, nr1, ni0, ni1 = load_parts(n_refs[b], w, groups)
                at = pl.ds((w * pairs + a * n_count + b) * groups, groups)
                for k, part in enumerate(
                    (
                        zr0 * nr0 + zi0 * ni0,
                        zr1 * nr1 + zi1 * ni1,
                        zi0 * nr0 - zr0 * ni0,
                        zi1 * nr1 - zr1 * ni1,
                    )
                ):
                    lhs_ref[at, k * LANES : (k + 1) * LANES] = part.astype(jnp.bfloat16)
    product = jnp.dot(lhs_ref[...], inner_ref[...], preferred_element_type=jnp.float32)
    turned = product.reshape(windows * pairs, groups, 2 * lags) * outer_ref[...][None]
    turned = jnp.sum(turned, 1)
    corr = turned[:, :lags] + turned[:, lags:]
    unit = corr / jnp.sqrt(jnp.mean(corr * corr, 1, keepdims=True) + 1e-05)

    z_marks = jnp.concatenate(
        [spread(zf_refs[a], 0, w, n_count) for w in range(windows) for a in range(z_count)]
    )
    n_marks = jnp.concatenate(
        [
            spread(nf_refs[b], 0, w, 1)
            for w in range(windows)
            for a in range(z_count)
            for b in range(n_count)
        ]
    )
    unit = unit * (z_marks * n_marks)[:, :1]
    stacked, count = unit[:pairs], (z_marks * n_marks)[:pairs]
    for w in range(1, windows):
        stacked = stacked + unit[w * pairs : (w + 1) * pairs]
        count = count + (z_marks * n_marks)[w * pairs : (w + 1) * pairs]
    stacked = stacked / jnp.maximum(count, 1.0)[:, :1]
    z_at = place(axes[0], z_count)
    n_at = place(axes[1], n_count)
    for a in range(z_count):
        for b in range(n_count):
            k = a * n_count + b
            rows_ref[pl.ds(z_at(a) * n_count + n_at(b), 1), :] = stacked[k : k + 1]
    mask = jnp.concatenate(
        [spread(mask_ref, a, b, 1) for a in range(z_count) for b in range(n_count)]
    )
    rows_ref[...] = rows_ref[...] * mask[:, :1]
    for a in range(z_count):
        out_ref[a] = rows_ref[a * n_count : (a + 1) * n_count]


WHOLE = pl.BlockSpec(memory_space=pltpu.VMEM)


def prepare(bins, lags, fine=16):
    t = np.arange(lags) - lags // 2

    def turns(s):
        angle = np.pi / bins * ((s[:, None] * t[None, :]) % (2 * bins))
        return jnp.asarray(np.concatenate([np.cos(angle), np.sin(angle)], 1), jnp.float32)

    return pl.pallas_call(
        functools.partial(prepare_kernel, bins // DEPTH, lags),
        out_shape=jax.ShapeDtypeStruct((2 * DEPTH, 2 * lags), jnp.bfloat16),
        in_specs=[WHOLE] * 2,
        out_specs=WHOLE,
        compiler_params=pltpu.CompilerParams(vmem_limit_bytes=4 << 20),
        cost_estimate=pl.CostEstimate(flops=8 << 20, bytes_accessed=1 << 20, transcendentals=0),
    )(turns(np.arange(0, DEPTH, fine)), turns(np.arange(fine)))


def outer_table(bins, lags):
    t = np.arange(lags) - lags // 2
    angle = np.pi / bins * ((DEPTH * np.arange(bins // DEPTH)[:, None] * t[None, :]) % (2 * bins))
    return jnp.asarray(2.0 * np.concatenate([np.cos(angle), -np.sin(angle)], 1), jnp.float32)


def correlate(axes, z_blocks, z_flags, n_blocks, n_flags, mask, inner, bins):
    z_count, n_count = len(z_blocks), len(n_blocks)
    windows = z_flags[0].shape[1]
    groups, pairs = bins // DEPTH, z_count * n_count
    return pl.pallas_call(
        functools.partial(correlate_kernel, axes, z_count, n_count, windows, groups, LAGS),
        out_shape=jax.ShapeDtypeStruct((z_count, n_count, LAGS), jnp.float32),
        in_specs=[WHOLE] * (2 * z_count + 2 * n_count + 3),
        out_specs=WHOLE,
        scratch_shapes=[
            pltpu.VMEM((windows * pairs * groups, 2 * DEPTH), jnp.bfloat16),
            pltpu.VMEM((pairs, LAGS), jnp.float32),
        ],
        compiler_params=pltpu.CompilerParams(vmem_limit_bytes=16 << 20),
        cost_estimate=pl.CostEstimate(flops=512 << 20, bytes_accessed=1 << 20, transcendentals=0),
    )(*z_blocks, *n_blocks, *z_flags, *n_flags, inner, outer_table(bins, LAGS), mask)


def as_rows(block):
    _, windows, parts, bins = block.shape
    block = block.reshape(windows, parts, bins // LANES, LANES)
    return jnp.swapaxes(block, 1, 2).reshape(windows * parts * bins // LANES, LANES)


def partners(size):
    if size & (size - 1) == 0:
        return [[(i, i ^ k) for i in range(size)] for k in range(1, size)]
    return [[(i, (i + k) % size) for i in range(size)] for k in range(1, size)]


def gather(block, axis, size):
    return [block] + [lax.ppermute(block, axis, to) for to in partners(size)]


def place(axis, size):
    if axis is None:
        return lambda k: k
    me = lax.axis_index(axis)
    if size & (size - 1) == 0:
        return lambda k: me ^ k
    return lambda k: lax.rem(me + size - k, size)


SMALL = 8


def body(sizes, z_spectra, n_spectra, z_flags, n_flags, pair_mask):
    bins = z_spectra.shape[-1]
    rows, cols = sizes
    z_own, n_own = as_rows(z_spectra), as_rows(n_spectra)
    inner = prepare(bins, LAGS)
    z_blocks, z_marks = gather(z_own, "col", cols), gather(z_flags, "col", cols)
    if rows <= SMALL:
        n_blocks, n_marks = gather(n_own, "row", rows), gather(n_flags, "row", rows)
        return correlate(
            ("col", "row"), z_blocks, z_marks, n_blocks, n_marks, pair_mask, inner, bins
        )
    n_all = lax.all_gather(n_own, "row", axis=0)
    n_marks = lax.all_gather(n_flags.astype(jnp.float32), "row", axis=0)
    step = math.gcd(rows, 4)
    count = rows // step

    def one(args):
        blocks, marks, mask = args
        return correlate(
            ("col", None), z_blocks, z_marks, list(blocks), list(marks), mask, inner, bins
        )

    stacks = lax.map(
        one,
        (
            n_all.reshape((count, step) + n_own.shape),
            n_marks.reshape((count, step) + n_flags.shape),
            jnp.moveaxis(pair_mask.reshape(-1, count, step), 1, 0),
        ),
    )
    return jnp.moveaxis(stacks, 0, 1).reshape(len(z_blocks), rows, LAGS)


def solution(mesh):
    placed = (
        P(("grp", "row", "col"), None, None, None),
        P(("grp", "col", "row"), None, None, None),
        P(("grp", "row", "col"), None),
        P(("grp", "col", "row"), None),
        P(("grp", "row"), "col"),
    )
    sizes = (mesh.shape["row"], mesh.shape["col"])
    return jax.shard_map(
        functools.partial(body, sizes),
        mesh=mesh,
        in_specs=placed,
        out_specs=P(("grp", "row"), "col", None),
        check_vma=False,
    )
```

```python
import functools
import math

import jax
import jax.numpy as jnp
import numpy as np
from jax import lax
from jax.experimental import pallas as pl
from jax.experimental.pallas import tpu as pltpu
from jax.sharding import PartitionSpec as P


LAGS = 512
LANES = 128
SUBLANES = 8
DEPTH = 2 * LANES
WHOLE = pl.BlockSpec(memory_space=pltpu.VMEM)
OPENF = 1 << 30

STAGES = ((0, 0, 0, 1), (0, 0, 0, 0))


def spread(ref, i, j, count=1):
    return jnp.broadcast_to(ref[i : i + 1, j : j + 1].astype(jnp.float32), (count, LANES))


def open_kernel(out_ref):
    out_ref[...] = jnp.zeros(out_ref.shape, out_ref.dtype)


def opening():
    return pl.pallas_call(
        open_kernel,
        out_shape=jax.ShapeDtypeStruct((SUBLANES, LANES), jnp.float32),
        out_specs=WHOLE,
        compiler_params=pltpu.CompilerParams(vmem_limit_bytes=1 << 20),
        cost_estimate=pl.CostEstimate(flops=OPENF, bytes_accessed=1 << 12, transcendentals=0),
    )()


def pack_kernel(block_ref, flag_ref, blank_ref, out_ref):
    rows, windows = block_ref.shape[0], flag_ref.shape[1]
    out_ref[:rows] = block_ref[...]
    lane = lax.broadcasted_iota(jnp.int32, (SUBLANES, LANES), 1)
    flags = blank_ref[...]
    for w in range(windows):
        flags = jnp.where(lane == w, spread(flag_ref, 0, w, SUBLANES), flags)
    out_ref[rows:] = flags


def pack(block, flags, blank):
    rows = block.shape[0]
    return pl.pallas_call(
        pack_kernel,
        out_shape=jax.ShapeDtypeStruct((rows + SUBLANES, LANES), jnp.float32),
        in_specs=[WHOLE] * 3,
        out_specs=WHOLE,
        compiler_params=pltpu.CompilerParams(vmem_limit_bytes=2 << 20),
    )(block, flags, blank)


def prepare_kernel(lags, coarse_ref, fine_ref, inner_ref):
    steps = fine_ref.shape[0]
    fine_cos, fine_sin = fine_ref[:, :lags], fine_ref[:, lags:]
    for k in range(coarse_ref.shape[0]):
        coarse_cos, coarse_sin = coarse_ref[k : k + 1, :lags], coarse_ref[k : k + 1, lags:]
        cos = (coarse_cos * fine_cos - coarse_sin * fine_sin).astype(jnp.bfloat16)
        sin = (coarse_sin * fine_cos + coarse_cos * fine_sin).astype(jnp.bfloat16)
        top, low = pl.ds(k * steps, steps), pl.ds(DEPTH + k * steps, steps)
        inner_ref[top, :lags] = cos
        inner_ref[top, lags:] = sin
        inner_ref[low, :lags] = (0.0 - sin.astype(jnp.float32)).astype(jnp.bfloat16)
        inner_ref[low, lags:] = cos


def turns(bins, lags, s):
    t = np.arange(lags) - lags // 2
    angle = np.pi / bins * ((s[:, None] * t[None, :]) % (2 * bins))
    return np.cos(angle), np.sin(angle)


def prepare(bins, lags, fine=16):
    near = [
        jnp.asarray(np.concatenate(turns(bins, lags, s), 1), jnp.float32)
        for s in (np.arange(0, DEPTH, fine), np.arange(fine))
    ]
    return pl.pallas_call(
        functools.partial(prepare_kernel, lags),
        out_shape=jax.ShapeDtypeStruct((2 * DEPTH, 2 * lags), jnp.bfloat16),
        in_specs=[WHOLE] * 2,
        out_specs=WHOLE,
        compiler_params=pltpu.CompilerParams(vmem_limit_bytes=4 << 20),
        cost_estimate=pl.CostEstimate(flops=8 << 20, bytes_accessed=1 << 20, transcendentals=0),
    )(*near)


def outer_table(bins, lags):
    cos, sin = turns(bins, lags, np.arange(0, bins, DEPTH))
    return jnp.asarray(2.0 * np.concatenate([cos, -sin], 1), jnp.float32)


def load_parts(ref, window, groups):
    base = window * 4 * groups
    return [ref[pl.ds(base + k, groups, stride=4), :] for k in (0, 2, 1, 3)]


def stack_pairs(windows, groups, lags, z_refs, n_refs, pairs, inner_ref, outer_ref, lhs_ref):
    row = lax.broadcasted_iota(jnp.int32, (groups, LANES), 0)
    lane = lax.broadcasted_iota(jnp.int32, (groups, LANES), 1)
    first = jnp.where((row == 0) & (lane == 0), 0.5, 1.0)
    count = len(pairs)
    for w in range(windows):
        for p, (a, b) in enumerate(pairs):
            zr0, zr1, zi0, zi1 = load_parts(z_refs[a], w, groups)
            zr0, zi0 = zr0 * first, zi0 * first
            nr0, nr1, ni0, ni1 = load_parts(n_refs[b], w, groups)
            parts = (
                zr0 * nr0 + zi0 * ni0,
                zr1 * nr1 + zi1 * ni1,
                zi0 * nr0 - zr0 * ni0,
                zi1 * nr1 - zr1 * ni1,
            )
            at = pl.ds((w * count + p) * groups, groups)
            for k, part in enumerate(parts):
                lhs_ref[at, k * LANES : (k + 1) * LANES] = part.astype(jnp.bfloat16)
    product = jnp.dot(lhs_ref[...], inner_ref[...], preferred_element_type=jnp.float32)
    turned = product.reshape(windows * count, groups, 2 * lags) * outer_ref[...][None]
    turned = jnp.sum(turned, 1)
    corr = turned[:, :lags] + turned[:, lags:]
    unit = corr / jnp.sqrt(jnp.mean(corr * corr, 1, keepdims=True) + 1e-05)
    flag_row = 4 * windows * groups
    marks = [
        jnp.concatenate([spread(z_refs[a], flag_row, w) for a, _ in pairs])
        * jnp.concatenate([spread(n_refs[b], flag_row, w) for _, b in pairs])
        for w in range(windows)
    ]
    total = sum(unit[w * count : (w + 1) * count] * marks[w][:, :1] for w in range(windows))
    return total / jnp.maximum(sum(marks), 1.0)[:, :1]


def stage_kernel(shape, lags, z_count, n_count, pairs, *refs):
    z_refs, n_refs = refs[:z_count], refs[z_count : z_count + n_count]
    inner_ref, outer_ref, out_ref, lhs_ref = refs[z_count + n_count :]
    out_ref[...] = stack_pairs(*shape, lags, z_refs, n_refs, pairs, inner_ref, outer_ref, lhs_ref)


def last_kernel(shape, lags, z_count, n_count, pairs, earlier, axes, *refs):
    z_refs, n_refs = refs[:z_count], refs[z_count : z_count + n_count]
    refs = refs[z_count + n_count :]
    done_refs, (inner_ref, outer_ref, mask_ref, out_ref, lhs_ref, rows_ref) = refs[:-6], refs[-6:]
    z_all, n_all = mask_ref.shape
    z_at, n_at = place(axes[0], z_all), place(axes[1], n_all)

    def put(a, b, row):
        rows_ref[pl.ds(z_at(a) * n_all + n_at(b), 1), :] = row

    for ref, slots in zip(done_refs, earlier):
        for k, (a, b) in enumerate(slots):
            put(a, b, ref[k : k + 1])
    mask = [
        jnp.concatenate([spread(mask_ref, a, b) for b in range(n_all)]) for a in range(z_all)
    ]
    local = [(pairs[0].index(a), pairs[1].index(b)) for a, b in pairs[2]]
    stacked = stack_pairs(*shape, lags, z_refs, n_refs, local, inner_ref, outer_ref, lhs_ref)
    for k, (a, b) in enumerate(pairs[2]):
        put(a, b, stacked[k : k + 1])
    for a in range(z_all):
        out_ref[a] = rows_ref[a * n_all : (a + 1) * n_all] * mask[a][:, :1]


def correlate(axes, stages, z_blocks, n_blocks, mask, inner, windows, bins):
    shape = (windows, bins // DEPTH)
    z_stage, n_stage = stages
    last = max(z_stage + n_stage)
    outer = outer_table(bins, LAGS)
    done, earlier = [], []
    for stage in range(last + 1):
        slots = [
            (a, b)
            for a in range(len(z_blocks))
            for b in range(len(n_blocks))
            if max(z_stage[a], n_stage[b]) == stage
        ]
        if not slots:
            continue
        z_used, n_used = (sorted(set(s)) for s in zip(*slots))
        count = len(slots)
        lhs = pltpu.VMEM((windows * count * shape[1], 2 * DEPTH), jnp.bfloat16)
        arrays = [z_blocks[a] for a in z_used] + [n_blocks[b] for b in n_used]
        settings = dict(
            out_specs=WHOLE,
            compiler_params=pltpu.CompilerParams(vmem_limit_bytes=16 << 20),
            cost_estimate=pl.CostEstimate(
                flops=count << 25, bytes_accessed=count << 16, transcendentals=0
            ),
        )
        if stage < last:
            local = [(z_used.index(a), n_used.index(b)) for a, b in slots]
            done.append(
                pl.pallas_call(
                    functools.partial(stage_kernel, shape, LAGS, len(z_used), len(n_used), local),
                    out_shape=jax.ShapeDtypeStruct((count, LAGS), jnp.float32),
                    in_specs=[WHOLE] * (len(arrays) + 2),
                    scratch_shapes=[lhs],
                    **settings,
                )(*arrays, inner, outer)
            )
            earlier.append(slots)
            continue
        used = (z_used, n_used, slots)
        return pl.pallas_call(
            functools.partial(
                last_kernel, shape, LAGS, len(z_used), len(n_used), used, earlier, axes
            ),
            out_shape=jax.ShapeDtypeStruct(mask.shape + (LAGS,), jnp.float32),
            in_specs=[WHOLE] * (len(arrays) + len(done) + 3),
            scratch_shapes=[lhs, pltpu.VMEM((mask.size, LAGS), jnp.float32)],
            **settings,
        )(*arrays, *done, inner, outer, mask)


def as_rows(block):
    _, windows, parts, bins = block.shape
    block = block.reshape(windows, parts, bins // LANES, LANES)
    return jnp.swapaxes(block, 1, 2).reshape(windows * parts * bins // LANES, LANES)


def two_way(size):
    return size & (size - 1) == 0


def partner(size, k):
    return [(i, i ^ k if two_way(size) else (i + k) % size) for i in range(size)]


def send(block, axis, size, k):
    return lax.ppermute(block, axis, partner(size, k))


def gather(block, axis, size):
    return [block] + [send(block, axis, size, k) for k in range(1, size)]


def gather_by_bits(block, axis, size):
    blocks, bit = {0: block}, size // 2
    while bit:
        for k in list(blocks):
            blocks[k | bit] = send(blocks[k], axis, size, bit)
        bit //= 2
    return [blocks[k] for k in range(size)]


def place(axis, size):
    if axis is None:
        return lambda k: k
    me = lax.axis_index(axis)
    if two_way(size):
        return lambda k: me ^ k
    return lambda k: lax.rem(me + size - k, size)


SMALL = 8


def body(sizes, z_spectra, n_spectra, z_flags, n_flags, pair_mask):
    return steps(sizes, z_spectra, n_spectra, z_flags, n_flags, pair_mask)


def steps(sizes, z_spectra, n_spectra, z_flags, n_flags, pair_mask):
    windows, bins = z_spectra.shape[1], z_spectra.shape[-1]
    rows, cols = sizes
    blank = opening()
    z_own = pack(as_rows(z_spectra), z_flags, blank)
    n_own = pack(as_rows(n_spectra), n_flags, blank)
    inner = prepare(bins, LAGS)
    z_blocks = gather_by_bits(z_own, "col", cols)
    if rows <= SMALL:
        n_blocks = gather(n_own, "row", rows)
        stages = STAGES if sizes == (4, 4) else ((0,) * cols, (0,) * rows)
        return correlate(
            ("col", "row"), stages, z_blocks, n_blocks, pair_mask, inner, windows, bins
        )
    n_all = lax.all_gather(n_own, "row", axis=0)
    step = math.gcd(rows, 4)
    count = rows // step
    stages = ((0,) * cols, (0,) * step)

    def one(args):
        blocks, mask = args
        return correlate(("col", None), stages, z_blocks, list(blocks), mask, inner, windows, bins)

    stacks = lax.map(
        one,
        (
            n_all.reshape((count, step) + n_own.shape),
            jnp.moveaxis(pair_mask.reshape(-1, count, step), 1, 0),
        ),
    )
    return jnp.moveaxis(stacks, 0, 1).reshape(cols, rows, LAGS)


def solution(mesh):
    placed = (
        P(("grp", "row", "col"), None, None, None),
        P(("grp", "col", "row"), None, None, None),
        P(("grp", "row", "col"), None),
        P(("grp", "col", "row"), None),
        P(("grp", "row"), "col"),
    )
    sizes = (mesh.shape["row"], mesh.shape["col"])
    return jax.shard_map(
        functools.partial(body, sizes),
        mesh=mesh,
        in_specs=placed,
        out_specs=P(("grp", "row"), "col", None),
        check_vma=False,
    )
```
